32 devices in a mesh: filt: 4 (over y, x), dom: 8 (over z, core).
Axes of the slice: x: 2, y: 2, z: 4, core: 2. Of those that a mesh axis runs over, the one named last changes fastest.
Arguments:
- log_weights: float32 [524288], P(('filt', 'dom')), parts along dimension 0, may hold values from -20 to 250, as said below
- bins: int32 [524288], P(('filt', 'dom')), parts along dimension 0, may hold values from 0 to 4095
- states: bfloat16 [128, 524288], P(None, ('filt', 'dom')), parts along dimension 1, may hold values from -6 to 6
Outputs:
- cumulative: float32 [16384], P(('filt', 'dom')), parts along dimension 0
- bin_means: float32 [128, 16384], P(None, ('filt', 'dom')), parts along dimension 1
- particle_weights: float32 [524288], P(('filt', 'dom')), parts along dimension 0
The draws below stay inside these ranges and needn't reach their ends.
There are 4 independent parts, one for each index of `filt`. The reference program is written for one: setup_inputs(seed, part) draws one part's arguments, and reference() takes and returns one part's arrays. A program takes and returns all parts, laid end to end along the dimension named above; each array names one. Nothing has to cross between parts.
Inputs may be any that keep to these rules, and one draw needn't show every extreme that they name: `log_weights`: finite log-weights.
All inputs are finite; a program needn't handle non-finite values.
Results may differ from the reference program's by a relative error of at most 0.00051.
Values sent between devices are 32-bit elements; how exact they have to be, the bound alone decides.
A program may use at most 64 MiB of HBM per device.

```python
import math
import jax
import jax.numpy as jnp
import numpy as np
from jax import lax

BINS = 4096
STATE = 128
P_DEV = 16384
PARTICLES = 131072
N_DOM = 8


def draw_log_weights(key, part):
    key_offset, key_noise = jax.random.split(jax.random.fold_in(key, 7))
    groups = PARTICLES // P_DEV
    offsets = jax.random.uniform(key_offset, (groups,), jnp.float32, -3.0, 3.0)
    noise = jnp.clip(1.5 * jax.random.normal(key_noise, (groups, P_DEV), jnp.float32), -8.0, 8.0)
    return (offsets[:, None] + noise).reshape(PARTICLES).astype(jnp.float32)


def set_ends(entries, stream_key, least, top_value):
    dims = entries.shape
    spot = [jax.random.randint(jax.random.fold_in(stream_key, axis), (), 0, dims[axis]) for axis in range(len(dims))]
    entries = entries.at[tuple(spot)].set(least)
    longest = dims.index(max(dims))
    spot[longest] = (spot[longest] + 1) % dims[longest]
    return entries.at[tuple(spot)].set(top_value)


def level_of(rng, dims, cuts, smallest, largest):
    gain = 1.0
    for axis_at, blocks in cuts:
        heights = jax.random.uniform(jax.random.fold_in(jax.random.fold_in(rng, 6), axis_at), (blocks,), jnp.float32, smallest / len(cuts), largest / len(cuts))
        gain = gain * jnp.repeat(jnp.exp(heights), dims[axis_at] // blocks).reshape((-1,) + (1,) * (len(dims) - 1 - axis_at))
    return gain


def rank_bounds(count, slope):
    weights = [(1 << 20) // math.isqrt(grade ** slope) + 1 for grade in range(1, count + 1)]
    scale = 1 + sum(weights) // (1 << 30)
    return np.cumsum(np.array([max(1, weight // scale) for weight in weights]))


def ranked(key, extent, amount, lean):
    table = rank_bounds(amount, lean)
    pick = jax.random.randint(jax.random.fold_in(key, 1), extent, 0, int(table[amount - 1]))
    rank = jnp.searchsorted(jnp.asarray(table, jnp.int32), pick, side="right")
    return jax.random.permutation(jax.random.fold_in(key, 2), amount)[rank].astype(jnp.int32)


def scatter_about(stream_key, dims, scale, limit, pieces=(), held_as=jnp.bfloat16):
    level = level_of(stream_key, dims, pieces, -0.22, 0.18) if pieces else 1.0
    entries = jax.random.normal(stream_key, dims, jnp.float32) * scale * level
    return jnp.minimum(jnp.maximum(entries, -limit), limit).astype(held_as)


def setup_inputs(seed: int = 0, part: int = 0) -> dict:
    key_of = jax.random.split(jax.random.key(seed), 4)
    part_splits = jax.random.split(jax.random.fold_in(key_of[3], part), 4)
    log_weights = draw_log_weights(jax.random.fold_in(jax.random.fold_in(key_of[3], part), 71), part)
    bins = set_ends(ranked(part_splits[1], (PARTICLES,), BINS, 2), jax.random.fold_in(part_splits[1], 3), 0, BINS - 1).astype(jnp.int32)
    states = scatter_about(part_splits[2], (STATE, PARTICLES), 1.0, 6.0, ((1, 8),))
    return dict(log_weights=log_weights, bins=bins, states=states)


floor_value = -1.0e4


def group_pairs(group_weights, group_bins, group_states):
    width = min(P_DEV, 1024)
    blocks = P_DEV // width
    labels = lax.iota(jnp.int32, BINS)

    def top_step(index, carry):
        start = (index * width).astype(jnp.int32)
        row_weights = lax.dynamic_slice_in_dim(group_weights, start, width)
        row_bins = lax.dynamic_slice_in_dim(group_bins, start, width)
        member = row_bins[:, None] == labels[None, :]
        return jnp.maximum(carry, jnp.max(jnp.where(member, row_weights[:, None], floor_value), axis=0))

    bin_top = lax.fori_loop(0, blocks, top_step, jnp.full((BINS,), floor_value, jnp.float32))

    def sum_step(index, carry):
        totals, sums = carry
        start = (index * width).astype(jnp.int32)
        row_weights = lax.dynamic_slice_in_dim(group_weights, start, width)
        row_bins = lax.dynamic_slice_in_dim(group_bins, start, width)
        row_states = lax.dynamic_slice_in_dim(group_states, start, width, 1).astype(jnp.float32)
        member = row_bins[:, None] == labels[None, :]
        own_top = jnp.sum(jnp.where(member, bin_top[None, :], jnp.float32(0.0)), axis=1)
        scaled = jnp.exp(row_weights - own_top).astype(jnp.bfloat16).astype(jnp.float32)
        spread = jnp.where(member, scaled[:, None], jnp.float32(0.0))
        totals = totals + jnp.sum(spread, axis=0)
        sums = sums + jnp.dot(row_states, spread, precision=lax.Precision.HIGHEST, preferred_element_type=jnp.float32)
        return totals, sums

    start_pair = (jnp.zeros((BINS,), jnp.float32), jnp.zeros((STATE, BINS), jnp.float32))
    totals, sums = lax.fori_loop(0, blocks, sum_step, start_pair)
    return bin_top, totals, sums


def reference(log_weights, bins, states):
    def one_group(group):
        start = (group * P_DEV).astype(jnp.int32)
        return group_pairs(lax.dynamic_slice_in_dim(log_weights, start, P_DEV),
                           lax.dynamic_slice_in_dim(bins, start, P_DEV),
                           lax.dynamic_slice_in_dim(states, start, P_DEV, 1))

    local_top, local_mass, local_sums = lax.map(one_group, jnp.arange(N_DOM, dtype=jnp.int32))
    bin_top = jnp.max(local_top, axis=0)
    factor = jnp.exp(local_top - bin_top[None, :])
    bin_mass = jnp.sum(local_mass * factor, axis=0)
    bin_sums = jnp.sum(local_sums * factor[:, None, :], axis=0)
    top = jnp.max(bin_top)
    share = bin_mass * jnp.exp(bin_top - top)
    total = jnp.sum(share)
    cumulative = jnp.cumsum(share) / total
    bin_means = bin_sums / jnp.maximum(bin_mass, 1.0)[None, :]
    particle_weights = (P_DEV * N_DOM) * jnp.exp(log_weights - top) / total
    return cumulative, bin_means, particle_weights
```

```python
import functools

import jax
import jax.numpy as jnp
from jax import lax
from jax.experimental import pallas as pl
from jax.experimental.pallas import tpu as pltpu
from jax.sharding import PartitionSpec as P

BINS = 4096
LANES = 128
EXTRA = 16

floor_value = -10000.0


def spread_rows(ref, values):
    for r in range(values.shape[0]):
        ref[16 * r:16 * r + 16, :] = jnp.broadcast_to(values[r:r + 1, :], (16, LANES)).astype(ref.dtype)


def local_tops(lw_t, bins_t):
    rows = lw_t.shape[1]
    tiles = BINS // LANES
    lane = lax.broadcasted_iota(jnp.int32, (8, LANES), 1)

    def step(r, acc):
        pick = jnp.full((LANES, LANES), r, jnp.int32)
        col_w = jnp.take_along_axis(lw_t, pick, axis=1).reshape(LANES // 8, 8, LANES)
        col_b = jnp.take_along_axis(bins_t, pick, axis=1).reshape(LANES // 8, 8, LANES)
        out = []
        for t in range(tiles):
            member = col_b == (lane + t * LANES)[None]
            out.append(jnp.maximum(acc[t], jnp.max(jnp.where(member, col_w, floor_value), axis=0)))
        return tuple(out)

    start = tuple(jnp.full((8, LANES), floor_value, jnp.float32) for _ in range(tiles))
    acc = lax.fori_loop(0, rows, step, start)
    return [jnp.max(a, axis=0, keepdims=True) for a in acc]


def merge(a, b, state):
    top_a, top_b = a[state + 8:state + 9], b[state + 8:state + 9]
    top = jnp.maximum(top_a, top_b)
    rows = a[0:state + 8] * jnp.exp(top_a - top) + b[0:state + 8] * jnp.exp(top_b - top)
    return rows, jnp.broadcast_to(top, (8, top.shape[1]))


def kernel(groups, whole_count, lw_ref, bins_ref, states_ref, cum_ref, means_ref, weights_ref,
           ext, lo_b, hi_b, w_b, top_tab, mine, pair_send, pair_recv, chip_send, chip_recv,
           stat_send, stat_recv, load_sem, pair_ss, pair_rs, chip_ss, chip_rs, stat_ss, stat_rs):
    state = states_ref.shape[0]
    count = states_ref.shape[1]
    rows = count // LANES
    owned = BINS // groups
    width = min(256, owned)
    chips = groups // 2
    me = lax.axis_index("dom")
    chip, core = me // 2, me % 2
    partner = chip * 2 + (1 - core)

    load = pltpu.make_async_copy(states_ref, ext.at[0:state], load_sem)
    load.start()
    barrier = pltpu.get_barrier_semaphore()
    for k in range(1, groups):
        pl.semaphore_signal(barrier, inc=1, device_id={"dom": lax.rem(me + k, groups)},
                            device_id_type=pl.DeviceIdType.MESH)

    ext[state:state + EXTRA, :] = jnp.ones((EXTRA, count), jnp.bfloat16)
    lw = lw_ref[...]
    bins = bins_ref[...]
    spread_rows(lo_b, (bins % width).astype(jnp.float32))
    spread_rows(hi_b, (bins // width).astype(jnp.float32))
    tops = local_tops(lw.T, bins.T)
    low, high = bins % LANES, bins // LANES
    own_top = jnp.zeros(lw.shape, jnp.float32)
    for t in range(BINS // LANES):
        picked = jnp.take_along_axis(jnp.broadcast_to(tops[t], lw.shape), low, axis=1)
        own_top = jnp.where(high == t, picked, own_top)
        top_tab[t] = jnp.broadcast_to(tops[t], (8, LANES))
    spread_rows(w_b, jnp.exp(lw - own_top))
    load.wait()
    pl.semaphore_wait(barrier, groups - 1)

    depth = 16
    label = lax.broadcasted_iota(jnp.int32, (width, LANES), 0).astype(jnp.float32).astype(jnp.bfloat16)
    zero = jnp.zeros((), jnp.bfloat16)

    def block(owner, out):
        for part in range(owned // width):
            tile = (owner * (owned // width) + part).astype(jnp.float32).astype(jnp.bfloat16)

            def step(c, acc):
                pieces = []
                for j in range(depth):
                    at = pl.ds(pl.multiple_of((c * depth + j) * 16, 16), 16)
                    w = jnp.where(hi_b[at, :] == tile, w_b[at, :], zero)
                    lo = lo_b[at, :]
                    w_all = jnp.concatenate([w] * (width // 16), axis=0)
                    lo_all = jnp.concatenate([lo] * (width // 16), axis=0)
                    pieces.append(jnp.where(lo_all == label, w_all, zero))
                spread = jnp.concatenate(pieces, axis=1)
                cols = pl.ds(pl.multiple_of(c * depth * LANES, LANES), depth * LANES)
                return acc + lax.dot_general(ext[:, cols], spread, (((1,), (1,)), ((), ())),
                                             preferred_element_type=jnp.float32)

            acc = lax.fori_loop(0, rows // depth, step, jnp.zeros((state + EXTRA, width), jnp.float32))
            out[:, part * width:(part + 1) * width] = acc
        for t in range(owned // LANES):
            out[state + 8:state + 16, t * LANES:(t + 1) * LANES] = top_tab[owner * (owned // LANES) + t]

    order = sorted(range(1, chips), key=lambda m: -min(m, chips - m)) + [0]
    pair_copies, chip_copies = [], []
    for s, m in enumerate(order):
        dest = lax.rem(chip + m, chips)
        block(dest * 2 + (1 - core), pair_send.at[s])
        copy = pltpu.make_async_remote_copy(
            pair_send.at[s], pair_recv.at[s], pair_ss.at[s], pair_rs.at[s],
            device_id={"dom": partner}, device_id_type=pl.DeviceIdType.MESH)
        copy.start()
        pair_copies.append(copy)
        block(dest * 2 + core, mine.at[s])
        copy.wait_recv()
        merged, top = merge(mine[s], pair_recv[s], state)
        chip_send[s, 0:state + 8, :] = merged
        chip_send[s, state + 8:state + 16, :] = top
        if m:
            copy = pltpu.make_async_remote_copy(
                chip_send.at[s], chip_recv.at[s], chip_ss.at[s], chip_rs.at[s],
                device_id={"dom": dest * 2 + core}, device_id_type=pl.DeviceIdType.MESH)
            copy.start()
            chip_copies.append(copy)

    for copy in chip_copies:
        copy.wait_recv()
    last = chips - 1
    tops = [chip_send[last, state + 8:state + 9, :]] + [chip_recv[s, state + 8:state + 9, :] for s in range(last)]
    bin_top = functools.reduce(jnp.maximum, tops)
    sums = chip_send[last, 0:state + 8, :] * jnp.exp(tops[0] - bin_top)
    for s in range(last):
        sums = sums + chip_recv[s, 0:state + 8, :] * jnp.exp(tops[s + 1] - bin_top)
    mass = sums[state:state + 1, :]
    block_top = jnp.max(bin_top, axis=1, keepdims=True)
    block_mass = jnp.sum(mass * jnp.exp(bin_top - block_top), axis=1, keepdims=True)
    stat_send[0:4, :] = jnp.broadcast_to(block_top, (4, LANES))
    stat_send[4:8, :] = jnp.broadcast_to(block_mass, (4, LANES))
    stat_copies = []
    for k in range(1, groups):
        copy = pltpu.make_async_remote_copy(
            stat_send, stat_recv.at[k - 1], stat_ss.at[k - 1], stat_rs.at[k - 1],
            device_id={"dom": lax.rem(me + k, groups)}, device_id_type=pl.DeviceIdType.MESH)
        copy.start()
        stat_copies.append(copy)
    means_ref[...] = sums[0:state] / jnp.maximum(mass, 1.0)
    for copy in stat_copies:
        copy.wait_recv()
    top = block_top
    for k in range(groups - 1):
        top = jnp.maximum(top, stat_recv[k, 0:1, 0:1])
    total = block_mass * jnp.exp(block_top - top)
    before = jnp.zeros_like(total)
    for k in range(groups - 1):
        theirs = stat_recv[k, 4:5, 0:1] * jnp.exp(stat_recv[k, 0:1, 0:1] - top)
        total = total + theirs
        before = before + jnp.where(me >= k + 1, theirs, 0.0)
    share = mass * jnp.exp(bin_top - top)
    position = lax.broadcasted_iota(jnp.int32, share.shape, 1)
    run = share
    hop = 1
    while hop < owned:
        run = run + jnp.where(position >= hop, pltpu.roll(run, hop, 1), 0.0)
        hop *= 2
    cum_ref[...] = (before + run) / total
    weights_ref[...] = whole_count * jnp.exp(lw - top) / total
    for copy in pair_copies + chip_copies + stat_copies:
        copy.wait_send()


def body(log_weights, bins, states):
    groups = lax.axis_size("dom")
    owned = BINS // groups
    chips = groups // 2
    state, count = states.shape
    rows = count // LANES
    vmem = pl.BlockSpec(memory_space=pltpu.VMEM)
    blocks = pltpu.VMEM((chips, state + EXTRA, owned), jnp.float32)
    cumulative, bin_means, weights = pl.pallas_call(
        functools.partial(kernel, groups, float(count * groups)),
        out_shape=(jax.ShapeDtypeStruct((1, owned), jnp.float32),
                   jax.ShapeDtypeStruct((state, owned), jnp.float32),
                   jax.ShapeDtypeStruct((rows, LANES), jnp.float32)),
        in_specs=[vmem, vmem, pl.BlockSpec(memory_space=pl.ANY)],
        out_specs=(vmem, vmem, vmem),
        scratch_shapes=[
            pltpu.VMEM((state + EXTRA, count), jnp.bfloat16),
            pltpu.VMEM((rows * 16, LANES), jnp.bfloat16),
            pltpu.VMEM((rows * 16, LANES), jnp.bfloat16),
            pltpu.VMEM((rows * 16, LANES), jnp.bfloat16),
            pltpu.VMEM((BINS // LANES, 8, LANES), jnp.float32),
            blocks, blocks, blocks, blocks, blocks,
            pltpu.VMEM((8, LANES), jnp.float32),
            pltpu.VMEM((groups - 1, 8, LANES), jnp.float32),
            pltpu.SemaphoreType.DMA,
            pltpu.SemaphoreType.DMA((chips,)),
            pltpu.SemaphoreType.DMA((chips,)),
            pltpu.SemaphoreType.DMA((chips,)),
            pltpu.SemaphoreType.DMA((chips,)),
            pltpu.SemaphoreType.DMA((groups - 1,)),
            pltpu.SemaphoreType.DMA((groups - 1,)),
        ],
        compiler_params=pltpu.CompilerParams(
            collective_id=0, has_side_effects=True, vmem_limit_bytes=48 * 1024 * 1024),
    )(log_weights.reshape(rows, LANES), bins.reshape(rows, LANES), states)
    return cumulative.reshape(owned), bin_means, weights.reshape(count)


def solution(mesh):
    placed = (P(("filt", "dom")), P(("filt", "dom")), P(None, ("filt", "dom")))
    return jax.shard_map(
        body,
        mesh=mesh,
        in_specs=placed,
        out_specs=(P(("filt", "dom")), P(None, ("filt", "dom")), P(("filt", "dom"))),
        check_vma=False,
    )
```

```python
import functools

import jax
import jax.numpy as jnp
from jax import lax
from jax.experimental import pallas as pl
from jax.experimental.pallas import tpu as pltpu
from jax.sharding import PartitionSpec as P

BINS = 4096
LANES = 128
EXTRA = 16

floor_value = -10000.0


def spread_rows(ref, values):
    for r in range(values.shape[0]):
        ref[16 * r:16 * r + 16, :] = jnp.broadcast_to(values[r:r + 1, :], (16, LANES)).astype(ref.dtype)


def local_tops(lw_t, bins_t):
    rows = lw_t.shape[1]
    tiles = BINS // LANES
    lane = lax.broadcasted_iota(jnp.int32, (8, LANES), 1)

    def step(r, acc):
        pick = jnp.full((LANES, LANES), r, jnp.int32)
        col_w = jnp.take_along_axis(lw_t, pick, axis=1).reshape(LANES // 8, 8, LANES)
        col_b = jnp.take_along_axis(bins_t, pick, axis=1).reshape(LANES // 8, 8, LANES)
        out = []
        for t in range(tiles):
            member = col_b == (lane + t * LANES)[None]
            out.append(jnp.maximum(acc[t], jnp.max(jnp.where(member, col_w, floor_value), axis=0)))
        return tuple(out)

    start = tuple(jnp.full((8, LANES), floor_value, jnp.float32) for _ in range(tiles))
    acc = lax.fori_loop(0, rows, step, start)
    return [jnp.max(a, axis=0, keepdims=True) for a in acc]


def kernel(groups, whole_count, lw_ref, bins_ref, states_ref, cum_ref, means_ref, weights_ref,
           held, ext, lo_b, hi_b, part_b, w_b, top_tab, blocks, pair_send, pair_recv, chip_send, chip_recv,
           stat_send, stat_recv, load_sem, pair_ss, pair_rs, chip_ss, chip_rs, stat_ss, stat_rs):
    state = states_ref.shape[0]
    count = states_ref.shape[1]
    rows = count // LANES
    owned = BINS // groups
    both = 2 * owned
    width = min(256, owned)
    split = both // width
    chips = groups // 2
    me = lax.axis_index("dom")
    chip, core = me // 2, me % 2
    partner = chip * 2 + (1 - core)

    load = pltpu.make_async_copy(states_ref, held, load_sem)
    load.start()
    barrier = pltpu.get_barrier_semaphore()
    for k in range(1, groups):
        pl.semaphore_signal(barrier, inc=1, device_id={"dom": lax.rem(me + k, groups)},
                            device_id_type=pl.DeviceIdType.MESH)

    lw = lw_ref[...]
    bins = bins_ref[...]
    spread_rows(lo_b, (bins % width).astype(jnp.float32))
    spread_rows(hi_b, (bins // both).astype(jnp.float32))
    spread_rows(part_b, ((bins % both) // width).astype(jnp.float32))
    tops = local_tops(lw.T, bins.T)
    low, high = bins % LANES, bins // LANES
    own_top = jnp.zeros(lw.shape, jnp.float32)
    for t in range(BINS // LANES):
        picked = jnp.take_along_axis(jnp.broadcast_to(tops[t], lw.shape), low, axis=1)
        own_top = jnp.where(high == t, picked, own_top)
        top_tab[t] = jnp.broadcast_to(tops[t], (8, LANES))
    spread_rows(w_b, jnp.exp(lw - own_top))
    load.wait()

    zero = jnp.zeros((), jnp.bfloat16)
    one_label = lax.broadcasted_iota(jnp.int32, (EXTRA, LANES), 0) // (EXTRA // split)
    one_label = one_label.astype(jnp.float32).astype(jnp.bfloat16)

    def mask_states(r, carry):
        part = part_b[pl.ds(pl.multiple_of(r * 16, 16), 16), :]
        cols = pl.ds(pl.multiple_of(r * LANES, LANES), LANES)
        tile = held[:, cols]
        part_all = jnp.concatenate([part] * (state // 16), axis=0)
        for q in range(split):
            ext[q * state:(q + 1) * state, cols] = jnp.where(part_all == jnp.bfloat16(q), tile, zero)
        ext[split * state:split * state + EXTRA, cols] = jnp.where(part == one_label, jnp.bfloat16(1), zero)
        return carry

    lax.fori_loop(0, rows, mask_states, 0)
    pl.semaphore_wait(barrier, groups - 1)

    depth = 16
    label = lax.broadcasted_iota(jnp.int32, (width, LANES), 0).astype(jnp.float32).astype(jnp.bfloat16)

    def block(dest, out):
        tile = dest.astype(jnp.float32).astype(jnp.bfloat16)

        def step(c, carry):
            pieces = []
            for j in range(depth):
                at = pl.ds(pl.multiple_of((c * depth + j) * 16, 16), 16)
                w = jnp.where(hi_b[at, :] == tile, w_b[at, :], zero)
                lo = lo_b[at, :]
                w_all = jnp.concatenate([w] * (width // 16), axis=0)
                lo_all = jnp.concatenate([lo] * (width // 16), axis=0)
                pieces.append(jnp.where(lo_all == label, w_all, zero))
            spread = jnp.concatenate(pieces, axis=1)
            cols = pl.ds(pl.multiple_of(c * depth * LANES, LANES), depth * LANES)
            out[...] += lax.dot_general(ext[:, cols], spread, (((1,), (1,)), ((), ())),
                                        preferred_element_type=jnp.float32)
            return carry

        out[...] = jnp.zeros(out.shape, jnp.float32)
        lax.fori_loop(0, rows // depth, step, 0)

    half = split // 2

    def part_of(found, which, p):
        sums = found[pl.ds(pl.multiple_of((which * half + p) * state, state), state), :]
        at = split * state + p * (EXTRA // split)
        first = found[at:at + 1, :]
        at = at + half * (EXTRA // split)
        return sums, jnp.where(which == 0, first, found[at:at + 1, :])

    def tops_of(owner, p):
        tiles = [top_tab[(owner * half + p) * (width // LANES) + t] for t in range(width // LANES)]
        return jnp.concatenate(tiles, axis=1)

    order = sorted(range(1, chips), key=lambda m: -min(m, chips - m)) + [0]
    pair_copies, chip_copies = [], []
    for s, m in enumerate(order):
        dest = lax.rem(chip + m, chips)
        found = blocks.at[s]
        block(dest, found)
        for p in range(half):
            lanes = slice(p * width, (p + 1) * width)
            sums, mass = part_of(found, 1 - core, p)
            pair_send[s, 0:state, lanes] = sums
            pair_send[s, state:state + 8, lanes] = jnp.broadcast_to(mass, (8, width))
            pair_send[s, state + 8:state + 16, lanes] = tops_of(dest * 2 + 1 - core, p)
        copy = pltpu.make_async_remote_copy(
            pair_send.at[s], pair_recv.at[s], pair_ss.at[s], pair_rs.at[s],
            device_id={"dom": partner}, device_id_type=pl.DeviceIdType.MESH)
        copy.start()
        pair_copies.append(copy)
        copy.wait_recv()
        for p in range(half):
            lanes = slice(p * width, (p + 1) * width)
            sums, mass = part_of(found, core, p)
            mine = tops_of(dest * 2 + core, p)
            theirs = pair_recv[s, state + 8:state + 16, lanes]
            top = jnp.maximum(mine, theirs)
            by_mine, by_theirs = jnp.exp(mine - top), jnp.exp(theirs - top)
            chip_send[s, 0:state, lanes] = sums * by_mine[0:1] + pair_recv[s, 0:state, lanes] * by_theirs[0:1]
            chip_send[s, state:state + 8, lanes] = mass * by_mine + pair_recv[s, state:state + 8, lanes] * by_theirs
            chip_send[s, state + 8:state + 16, lanes] = top
        if m:
            copy = pltpu.make_async_remote_copy(
                chip_send.at[s], chip_recv.at[s], chip_ss.at[s], chip_rs.at[s],
                device_id={"dom": dest * 2 + core}, device_id_type=pl.DeviceIdType.MESH)
            copy.start()
            chip_copies.append(copy)

    for copy in chip_copies:
        copy.wait_recv()
    last = chips - 1
    tops = [chip_send[last, state + 8:state + 9, :]] + [chip_recv[s, state + 8:state + 9, :] for s in range(last)]
    bin_top = functools.reduce(jnp.maximum, tops)
    sums = chip_send[last, 0:state + 8, :] * jnp.exp(tops[0] - bin_top)
    for s in range(last):
        sums = sums + chip_recv[s, 0:state + 8, :] * jnp.exp(tops[s + 1] - bin_top)
    mass = sums[state:state + 1, :]
    block_top = jnp.max(bin_top, axis=1, keepdims=True)
    block_mass = jnp.sum(mass * jnp.exp(bin_top - block_top), axis=1, keepdims=True)
    stat_send[0:4, :] = jnp.broadcast_to(block_top, (4, LANES))
    stat_send[4:8, :] = jnp.broadcast_to(block_mass, (4, LANES))
    stat_copies = []
    for k in range(1, groups):
        copy = pltpu.make_async_remote_copy(
            stat_send, stat_recv.at[k - 1], stat_ss.at[k - 1], stat_rs.at[k - 1],
            device_id={"dom": lax.rem(me + k, groups)}, device_id_type=pl.DeviceIdType.MESH)
        copy.start()
        stat_copies.append(copy)
    means_ref[...] = sums[0:state] / jnp.maximum(mass, 1.0)
    for copy in stat_copies:
        copy.wait_recv()
    top = block_top
    for k in range(groups - 1):
        top = jnp.maximum(top, stat_recv[k, 0:1, 0:1])
    total = block_mass * jnp.exp(block_top - top)
    before = jnp.zeros_like(total)
    for k in range(groups - 1):
        theirs = stat_recv[k, 4:5, 0:1] * jnp.exp(stat_recv[k, 0:1, 0:1] - top)
        total = total + theirs
        before = before + jnp.where(me >= k + 1, theirs, 0.0)
    share = mass * jnp.exp(bin_top - top)
    position = lax.broadcasted_iota(jnp.int32, share.shape, 1)
    run = share
    hop = 1
    while hop < owned:
        run = run + jnp.where(position >= hop, pltpu.roll(run, hop, 1), 0.0)
        hop *= 2
    cum_ref[...] = (before + run) / total
    weights_ref[...] = whole_count * jnp.exp(lw - top) / total
    for copy in pair_copies + chip_copies + stat_copies:
        copy.wait_send()


def body(log_weights, bins, states):
    groups = lax.axis_size("dom")
    owned = BINS // groups
    chips = groups // 2
    state, count = states.shape
    rows = count // LANES
    width = min(256, owned)
    split = 2 * owned // width
    vmem = pl.BlockSpec(memory_space=pltpu.VMEM)
    blocks = pltpu.VMEM((chips, state + EXTRA, owned), jnp.float32)
    cumulative, bin_means, weights = pl.pallas_call(
        functools.partial(kernel, groups, float(count * groups)),
        out_shape=(jax.ShapeDtypeStruct((1, owned), jnp.float32),
                   jax.ShapeDtypeStruct((state, owned), jnp.float32),
                   jax.ShapeDtypeStruct((rows, LANES), jnp.float32)),
        in_specs=[vmem, vmem, pl.BlockSpec(memory_space=pl.ANY)],
        out_specs=(vmem, vmem, vmem),
        scratch_shapes=[
            pltpu.VMEM((state, count), jnp.bfloat16),
            pltpu.VMEM((split * state + EXTRA, count), jnp.bfloat16),
            pltpu.VMEM((rows * 16, LANES), jnp.bfloat16),
            pltpu.VMEM((rows * 16, LANES), jnp.bfloat16),
            pltpu.VMEM((rows * 16, LANES), jnp.bfloat16),
            pltpu.VMEM((rows * 16, LANES), jnp.bfloat16),
            pltpu.VMEM((BINS // LANES, 8, LANES), jnp.float32),
            pltpu.VMEM((chips, split * state + EXTRA, width), jnp.float32),
            blocks, blocks, blocks, blocks,
            pltpu.VMEM((8, LANES), jnp.float32),
            pltpu.VMEM((groups - 1, 8, LANES), jnp.float32),
            pltpu.SemaphoreType.DMA,
            pltpu.SemaphoreType.DMA((chips,)),
            pltpu.SemaphoreType.DMA((chips,)),
            pltpu.SemaphoreType.DMA((chips,)),
            pltpu.SemaphoreType.DMA((chips,)),
            pltpu.SemaphoreType.DMA((groups - 1,)),
            pltpu.SemaphoreType.DMA((groups - 1,)),
        ],
        compiler_params=pltpu.CompilerParams(
            collective_id=0, has_side_effects=True, vmem_limit_bytes=48 * 1024 * 1024),
    )(log_weights.reshape(rows, LANES), bins.reshape(rows, LANES), states)
    return cumulative.reshape(owned), bin_means, weights.reshape(count)


def solution(mesh):
    placed = (P(("filt", "dom")), P(("filt", "dom")), P(None, ("filt", "dom")))
    return jax.shard_map(
        body,
        mesh=mesh,
        in_specs=placed,
        out_specs=(P(("filt", "dom")), P(None, ("filt", "dom")), P(("filt", "dom"))),
        check_vma=False,
    )
```

```python
import functools

import jax
import jax.numpy as jnp
from jax import lax
from jax.experimental import pallas as pl
from jax.experimental.pallas import tpu as pltpu
from jax.sharding import PartitionSpec as P

BINS = 4096
LANES = 128
EXTRA = 16

floor_value = -10000.0


def spread_rows(ref, values):
    for r in range(values.shape[0]):
        ref[16 * r:16 * r + 16, :] = jnp.broadcast_to(values[r:r + 1, :], (16, LANES)).astype(ref.dtype)


def sort_pairs(keys, values):
    tile_bits = len(keys).bit_length() - 1
    bits = tile_bits + 10
    sub = lax.broadcasted_iota(jnp.int32, (8, LANES), 0)
    lane = lax.broadcasted_iota(jnp.int32, (8, LANES), 1)

    def mask_of(bit):
        if bit < tile_bits + 3:
            return (sub & (1 << (bit - tile_bits))) != 0
        return (lane & (1 << (bit - tile_bits - 3))) != 0

    def after(ka, va, kb, vb):
        return (ka > kb) | ((ka == kb) & (va > vb))

    for size in range(1, bits + 1):
        for bit in range(size - 1, -1, -1):
            down = mask_of(size) if tile_bits <= size < bits else None
            if bit < tile_bits:
                for t in range(len(keys)):
                    o = t | (1 << bit)
                    if o == t:
                        continue
                    swap = after(keys[t], values[t], keys[o], values[o])
                    if down is not None:
                        swap = jnp.logical_xor(swap, down)
                    elif size < tile_bits and t & (1 << size):
                        swap = after(keys[o], values[o], keys[t], values[t])
                    keys[t], keys[o] = jnp.where(swap, keys[o], keys[t]), jnp.where(swap, keys[t], keys[o])
                    values[t], values[o] = (jnp.where(swap, values[o], values[t]),
                                            jnp.where(swap, values[t], values[o]))
                continue
            upper = mask_of(bit)
            turn = upper if down is None else jnp.logical_xor(upper, down)
            if bit < tile_bits + 3:
                hop = 1 << (bit - tile_bits)

                def partner(x):
                    if 2 * hop == 8:
                        return pltpu.roll(x, hop, 0)
                    return jnp.where(upper, pltpu.roll(x, hop, 0), pltpu.roll(x, 8 - hop, 0))
            else:
                index = lane ^ (1 << (bit - tile_bits - 3))

                def partner(x):
                    return jnp.take_along_axis(x, index, axis=1)
            for t in range(len(keys)):
                k, v = partner(keys[t]), partner(values[t])
                swap = jnp.logical_xor(after(keys[t], values[t], k, v), turn)
                keys[t] = jnp.where(swap, k, keys[t])
                values[t] = jnp.where(swap, v, values[t])
    return keys, values


def local_tops(lw, bins):
    count = lw.shape[0] // 8
    table = BINS // LANES
    keys, values = sort_pairs([bins[8 * t:8 * t + 8] for t in range(count)],
                              [lw[8 * t:8 * t + 8] for t in range(count)])
    sub = lax.broadcasted_iota(jnp.int32, (8, LANES), 0)
    lane = lax.broadcasted_iota(jnp.int32, (8, LANES), 1)
    turned = pltpu.roll(keys[0], 7, 0)
    following = jnp.where(sub == 7, pltpu.roll(turned, LANES - 1, 1), turned)
    following = jnp.where((sub == 7) & (lane == LANES - 1), -1, following)
    high_label = lax.broadcasted_iota(jnp.int32, (table, LANES), 0)
    low_label = lax.broadcasted_iota(jnp.int32, (LANES, LANES), 0)
    found = jnp.zeros((4 * table, LANES), jnp.float32)
    for t in range(count):
        last = keys[t] != (keys[t + 1] if t + 1 < count else following)
        high = jnp.where(last, keys[t] // LANES, -1)
        low = keys[t] % LANES
        first = values[t].astype(jnp.bfloat16).astype(jnp.float32)
        rest = values[t] - first
        second = rest.astype(jnp.bfloat16).astype(jnp.float32)
        third = rest - second
        left, right = [], []
        for r in range(8):
            member = high[r:r + 1] == high_label
            pieces = [jnp.where(member, x[r:r + 1], 0.0) for x in (first, second, third)]
            pieces.append(jnp.where(member, 1.0, 0.0))
            left.append(jnp.concatenate(pieces, axis=0).astype(jnp.bfloat16))
            right.append(jnp.where(low[r:r + 1] == low_label, 1.0, 0.0).astype(jnp.bfloat16))
        found = found + lax.dot_general(jnp.concatenate(left, axis=1), jnp.concatenate(right, axis=1),
                                        (((1,), (1,)), ((), ())), preferred_element_type=jnp.float32)
    top = (found[0:table] + found[table:2 * table]) + found[2 * table:3 * table]
    return jnp.where(found[3 * table:] > 0.5, top, floor_value)


def kernel(groups, whole_count, lw_ref, bins_ref, states_ref, cum_ref, means_ref, weights_ref,
           held, ext, lo_b, hi_b, part_b, w_b, top_tab, blocks, pair_send, pair_recv, chip_send, chip_recv,
           stat_send, stat_recv, load_sem, pair_ss, pair_rs, chip_ss, chip_rs, stat_ss, stat_rs):
    state = states_ref.shape[0]
    count = states_ref.shape[1]
    rows = count // LANES
    owned = BINS // groups
    both = 2 * owned
    width = min(256, owned)
    split = both // width
    chips = groups // 2
    me = lax.axis_index("dom")
    chip, core = me // 2, me % 2
    partner = chip * 2 + (1 - core)

    load = pltpu.make_async_copy(states_ref, held, load_sem)
    load.start()
    barrier = pltpu.get_barrier_semaphore()
    for k in range(1, groups):
        pl.semaphore_signal(barrier, inc=1, device_id={"dom": lax.rem(me + k, groups)},
                            device_id_type=pl.DeviceIdType.MESH)

    lw = lw_ref[...]
    bins = bins_ref[...]
    spread_rows(lo_b, (bins % width).astype(jnp.float32))
    spread_rows(hi_b, (bins // both).astype(jnp.float32))
    spread_rows(part_b, ((bins % both) // width).astype(jnp.float32))
    tops = local_tops(lw, bins)
    low, high = bins % LANES, bins // LANES
    own_top = jnp.zeros(lw.shape, jnp.float32)
    for t in range(BINS // LANES):
        picked = jnp.take_along_axis(jnp.broadcast_to(tops[t:t + 1], lw.shape), low, axis=1)
        own_top = jnp.where(high == t, picked, own_top)
        top_tab[t] = jnp.broadcast_to(tops[t:t + 1], (8, LANES))
    spread_rows(w_b, jnp.exp(lw - own_top))
    load.wait()

    zero = jnp.zeros((), jnp.bfloat16)
    one_label = lax.broadcasted_iota(jnp.int32, (EXTRA, LANES), 0) // (EXTRA // split)
    one_label = one_label.astype(jnp.float32).astype(jnp.bfloat16)

    def mask_states(r, carry):
        part = part_b[pl.ds(pl.multiple_of(r * 16, 16), 16), :]
        cols = pl.ds(pl.multiple_of(r * LANES, LANES), LANES)
        tile = held[:, cols]
        part_all = jnp.concatenate([part] * (state // 16), axis=0)
        for q in range(split):
            ext[q * state:(q + 1) * state, cols] = jnp.where(part_all == jnp.bfloat16(q), tile, zero)
        ext[split * state:split * state + EXTRA, cols] = jnp.where(part == one_label, jnp.bfloat16(1), zero)
        return carry

    lax.fori_loop(0, rows, mask_states, 0)
    pl.semaphore_wait(barrier, groups - 1)

    depth = 16
    label = lax.broadcasted_iota(jnp.int32, (width, LANES), 0).astype(jnp.float32).astype(jnp.bfloat16)

    def block(dest, out):
        tile = dest.astype(jnp.float32).astype(jnp.bfloat16)

        def step(c, carry):
            pieces = []
            for j in range(depth):
                at = pl.ds(pl.multiple_of((c * depth + j) * 16, 16), 16)
                w = jnp.where(hi_b[at, :] == tile, w_b[at, :], zero)
                lo = lo_b[at, :]
                w_all = jnp.concatenate([w] * (width // 16), axis=0)
                lo_all = jnp.concatenate([lo] * (width // 16), axis=0)
                pieces.append(jnp.where(lo_all == label, w_all, zero))
            spread = jnp.concatenate(pieces, axis=1)
            cols = pl.ds(pl.multiple_of(c * depth * LANES, LANES), depth * LANES)
            out[...] += lax.dot_general(ext[:, cols], spread, (((1,), (1,)), ((), ())),
                                        preferred_element_type=jnp.float32)
            return carry

        out[...] = jnp.zeros(out.shape, jnp.float32)
        lax.fori_loop(0, rows // depth, step, 0)

    half = split // 2

    def part_of(found, which, p):
        sums = found[pl.ds(pl.multiple_of((which * half + p) * state, state), state), :]
        at = split * state + p * (EXTRA // split)
        first = found[at:at + 1, :]
        at = at + half * (EXTRA // split)
        return sums, jnp.where(which == 0, first, found[at:at + 1, :])

    def tops_of(owner, p):
        tiles = [top_tab[(owner * half + p) * (width // LANES) + t] for t in range(width // LANES)]
        return jnp.concatenate(tiles, axis=1)

    order = sorted(range(1, chips), key=lambda m: -min(m, chips - m)) + [0]
    pair_copies, chip_copies = [], []
    for s, m in enumerate(order):
        dest = lax.rem(chip + m, chips)
        found = blocks.at[s]
        block(dest, found)
        for p in range(half):
            lanes = slice(p * width, (p + 1) * width)
            sums, mass = part_of(found, 1 - core, p)
            pair_send[s, 0:state, lanes] = sums
            pair_send[s, state:state + 8, lanes] = jnp.broadcast_to(mass, (8, width))
            pair_send[s, state + 8:state + 16, lanes] = tops_of(dest * 2 + 1 - core, p)
        copy = pltpu.make_async_remote_copy(
            pair_send.at[s], pair_recv.at[s], pair_ss.at[s], pair_rs.at[s],
            device_id={"dom": partner}, device_id_type=pl.DeviceIdType.MESH)
        copy.start()
        pair_copies.append(copy)
        copy.wait_recv()
        for p in range(half):
            lanes = slice(p * width, (p + 1) * width)
            sums, mass = part_of(found, core, p)
            mine = tops_of(dest * 2 + core, p)
            theirs = pair_recv[s, state + 8:state + 16, lanes]
            top = jnp.maximum(mine, theirs)
            by_mine, by_theirs = jnp.exp(mine - top), jnp.exp(theirs - top)
            chip_send[s, 0:state, lanes] = sums * by_mine[0:1] + pair_recv[s, 0:state, lanes] * by_theirs[0:1]
            chip_send[s, state:state + 8, lanes] = mass * by_mine + pair_recv[s, state:state + 8, lanes] * by_theirs
            chip_send[s, state + 8:state + 16, lanes] = top
        if m:
            copy = pltpu.make_async_remote_copy(
                chip_send.at[s], chip_recv.at[s], chip_ss.at[s], chip_rs.at[s],
                device_id={"dom": dest * 2 + core}, device_id_type=pl.DeviceIdType.MESH)
            copy.start()
            chip_copies.append(copy)

    for copy in chip_copies:
        copy.wait_recv()
    last = chips - 1
    tops = [chip_send[last, state + 8:state + 9, :]] + [chip_recv[s, state + 8:state + 9, :] for s in range(last)]
    bin_top = functools.reduce(jnp.maximum, tops)
    sums = chip_send[last, 0:state + 8, :] * jnp.exp(tops[0] - bin_top)
    for s in range(last):
        sums = sums + chip_recv[s, 0:state + 8, :] * jnp.exp(tops[s + 1] - bin_top)
    mass = sums[state:state + 1, :]
    block_top = jnp.max(bin_top, axis=1, keepdims=True)
    block_mass = jnp.sum(mass * jnp.exp(bin_top - block_top), axis=1, keepdims=True)
    stat_send[0:4, :] = jnp.broadcast_to(block_top, (4, LANES))
    stat_send[4:8, :] = jnp.broadcast_to(block_mass, (4, LANES))
    stat_copies = []
    for k in range(1, groups):
        copy = pltpu.make_async_remote_copy(
            stat_send, stat_recv.at[k - 1], stat_ss.at[k - 1], stat_rs.at[k - 1],
            device_id={"dom": lax.rem(me + k, groups)}, device_id_type=pl.DeviceIdType.MESH)
        copy.start()
        stat_copies.append(copy)
    means_ref[...] = sums[0:state] / jnp.maximum(mass, 1.0)
    for copy in stat_copies:
        copy.wait_recv()
    top = block_top
    for k in range(groups - 1):
        top = jnp.maximum(top, stat_recv[k, 0:1, 0:1])
    total = block_mass * jnp.exp(block_top - top)
    before = jnp.zeros_like(total)
    for k in range(groups - 1):
        theirs = stat_recv[k, 4:5, 0:1] * jnp.exp(stat_recv[k, 0:1, 0:1] - top)
        total = total + theirs
        before = before + jnp.where(me >= k + 1, theirs, 0.0)
    share = mass * jnp.exp(bin_top - top)
    position = lax.broadcasted_iota(jnp.int32, share.shape, 1)
    run = share
    hop = 1
    while hop < owned:
        run = run + jnp.where(position >= hop, pltpu.roll(run, hop, 1), 0.0)
        hop *= 2
    cum_ref[...] = (before + run) / total
    weights_ref[...] = whole_count * jnp.exp(lw - top) / total
    for copy in pair_copies + chip_copies + stat_copies:
        copy.wait_send()


def body(log_weights, bins, states):
    groups = lax.axis_size("dom")
    owned = BINS // groups
    chips = groups // 2
    state, count = states.shape
    rows = count // LANES
    width = min(256, owned)
    split = 2 * owned // width
    vmem = pl.BlockSpec(memory_space=pltpu.VMEM)
    blocks = pltpu.VMEM((chips, state + EXTRA, owned), jnp.float32)
    cumulative, bin_means, weights = pl.pallas_call(
        functools.partial(kernel, groups, float(count * groups)),
        out_shape=(jax.ShapeDtypeStruct((1, owned), jnp.float32),
                   jax.ShapeDtypeStruct((state, owned), jnp.float32),
                   jax.ShapeDtypeStruct((rows, LANES), jnp.float32)),
        in_specs=[vmem, vmem, pl.BlockSpec(memory_space=pl.ANY)],
        out_specs=(vmem, vmem, vmem),
        scratch_shapes=[
            pltpu.VMEM((state, count), jnp.bfloat16),
            pltpu.VMEM((split * state + EXTRA, count), jnp.bfloat16),
            pltpu.VMEM((rows * 16, LANES), jnp.bfloat16),
            pltpu.VMEM((rows * 16, LANES), jnp.bfloat16),
            pltpu.VMEM((rows * 16, LANES), jnp.bfloat16),
            pltpu.VMEM((rows * 16, LANES), jnp.bfloat16),
            pltpu.VMEM((BINS // LANES, 8, LANES), jnp.float32),
            pltpu.VMEM((chips, split * state + EXTRA, width), jnp.float32),
            blocks, blocks, blocks, blocks,
            pltpu.VMEM((8, LANES), jnp.float32),
            pltpu.VMEM((groups - 1, 8, LANES), jnp.float32),
            pltpu.SemaphoreType.DMA,
            pltpu.SemaphoreType.DMA((chips,)),
            pltpu.SemaphoreType.DMA((chips,)),
            pltpu.SemaphoreType.DMA((chips,)),
            pltpu.SemaphoreType.DMA((chips,)),
            pltpu.SemaphoreType.DMA((groups - 1,)),
            pltpu.SemaphoreType.DMA((groups - 1,)),
        ],
        compiler_params=pltpu.CompilerParams(
            collective_id=0, has_side_effects=True, vmem_limit_bytes=48 * 1024 * 1024),
    )(log_weights.reshape(rows, LANES), bins.reshape(rows, LANES), states)
    return cumulative.reshape(owned), bin_means, weights.reshape(count)


def solution(mesh):
    placed = (P(("filt", "dom")), P(("filt", "dom")), P(None, ("filt", "dom")))
    return jax.shard_map(
        body,
        mesh=mesh,
        in_specs=placed,
        out_specs=(P(("filt", "dom")), P(None, ("filt", "dom")), P(("filt", "dom"))),
        check_vma=False,
    )
```

```python
import functools

import jax
import jax.numpy as jnp
from jax import lax
from jax.experimental import pallas as pl
from jax.experimental.pallas import tpu as pltpu
from jax.sharding import PartitionSpec as P

BINS = 4096
LANES = 128
EXTRA = 16

floor_value = -10000.0


def spread_rows(ref, values):
    for r in range(values.shape[0]):
        ref[16 * r:16 * r + 16, :] = jnp.broadcast_to(values[r:r + 1, :], (16, LANES)).astype(ref.dtype)


def sort_pairs(keys, values):
    tile_bits = len(keys).bit_length() - 1
    bits = tile_bits + 10
    sub = lax.broadcasted_iota(jnp.int32, (8, LANES), 0)
    lane = lax.broadcasted_iota(jnp.int32, (8, LANES), 1)

    def mask_of(bit):
        if bit < tile_bits + 3:
            return (sub & (1 << (bit - tile_bits))) != 0
        return (lane & (1 << (bit - tile_bits - 3))) != 0

    def after(ka, va, kb, vb):
        return (ka > kb) | ((ka == kb) & (va > vb))

    for size in range(1, bits + 1):
        for bit in range(size - 1, -1, -1):
            down = mask_of(size) if tile_bits <= size < bits else None
            if bit < tile_bits:
                for t in range(len(keys)):
                    o = t | (1 << bit)
                    if o == t:
                        continue
                    swap = after(keys[t], values[t], keys[o], values[o])
                    if down is not None:
                        swap = jnp.logical_xor(swap, down)
                    elif size < tile_bits and t & (1 << size):
                        swap = after(keys[o], values[o], keys[t], values[t])
                    keys[t], keys[o] = jnp.where(swap, keys[o], keys[t]), jnp.where(swap, keys[t], keys[o])
                    values[t], values[o] = (jnp.where(swap, values[o], values[t]),
                                            jnp.where(swap, values[t], values[o]))
                continue
            upper = mask_of(bit)
            turn = upper if down is None else jnp.logical_xor(upper, down)
            if bit < tile_bits + 3:
                hop = 1 << (bit - tile_bits)

                def partner(x):
                    if 2 * hop == 8:
                        return pltpu.roll(x, hop, 0)
                    return jnp.where(upper, pltpu.roll(x, hop, 0), pltpu.roll(x, 8 - hop, 0))
            else:
                index = lane ^ (1 << (bit - tile_bits - 3))

                def partner(x):
                    return jnp.take_along_axis(x, index, axis=1)
            for t in range(len(keys)):
                k, v = partner(keys[t]), partner(values[t])
                swap = jnp.logical_xor(after(keys[t], values[t], k, v), turn)
                keys[t] = jnp.where(swap, k, keys[t])
                values[t] = jnp.where(swap, v, values[t])
    return keys, values


def local_tops(lw, bins):
    count = lw.shape[0] // 8
    table = BINS // LANES
    keys, values = sort_pairs([bins[8 * t:8 * t + 8] for t in range(count)],
                              [lw[8 * t:8 * t + 8] for t in range(count)])
    sub = lax.broadcasted_iota(jnp.int32, (8, LANES), 0)
    lane = lax.broadcasted_iota(jnp.int32, (8, LANES), 1)
    turned = pltpu.roll(keys[0], 7, 0)
    following = jnp.where(sub == 7, pltpu.roll(turned, LANES - 1, 1), turned)
    following = jnp.where((sub == 7) & (lane == LANES - 1), -1, following)
    high_label = lax.broadcasted_iota(jnp.int32, (table, LANES), 0)
    low_label = lax.broadcasted_iota(jnp.int32, (LANES, LANES), 0)
    found = jnp.zeros((4 * table, LANES), jnp.float32)
    for t in range(count):
        last = keys[t] != (keys[t + 1] if t + 1 < count else following)
        high = jnp.where(last, keys[t] // LANES, -1)
        low = keys[t] % LANES
        first = values[t].astype(jnp.bfloat16).astype(jnp.float32)
        rest = values[t] - first
        second = rest.astype(jnp.bfloat16).astype(jnp.float32)
        third = rest - second
        left, right = [], []
        for r in range(8):
            member = high[r:r + 1] == high_label
            pieces = [jnp.where(member, x[r:r + 1], 0.0) for x in (first, second, third)]
            pieces.append(jnp.where(member, 1.0, 0.0))
            left.append(jnp.concatenate(pieces, axis=0).astype(jnp.bfloat16))
            right.append(jnp.where(low[r:r + 1] == low_label, 1.0, 0.0).astype(jnp.bfloat16))
        found = found + lax.dot_general(jnp.concatenate(left, axis=1), jnp.concatenate(right, axis=1),
                                        (((1,), (1,)), ((), ())), preferred_element_type=jnp.float32)
    top = (found[0:table] + found[table:2 * table]) + found[2 * table:3 * table]
    return jnp.where(found[3 * table:] > 0.5, top, floor_value)


def kernel(groups, whole_count, lw_ref, bins_ref, states_ref, cum_ref, means_ref, weights_ref,
           held, ext, lo_b, hi_b, part_b, w_b, top_tab, blocks, pair_send, pair_recv, chip_send, chip_recv,
           stat_send, stat_recv, load_sem, pair_ss, pair_rs, chip_ss, chip_rs, stat_ss, stat_rs):
    state = states_ref.shape[0]
    count = states_ref.shape[1]
    rows = count // LANES
    owned = BINS // groups
    both = 2 * owned
    width = min(256, owned)
    split = both // width
    chips = groups // 2
    me = lax.axis_index("dom")
    chip, core = me // 2, me % 2
    partner = chip * 2 + (1 - core)

    load = pltpu.make_async_copy(states_ref, held, load_sem)
    load.start()
    barrier = pltpu.get_barrier_semaphore()
    for k in range(1, groups):
        pl.semaphore_signal(barrier, inc=1, device_id={"dom": lax.rem(me + k, groups)},
                            device_id_type=pl.DeviceIdType.MESH)

    lw = lw_ref[...]
    bins = bins_ref[...]
    spread_rows(lo_b, (bins % width).astype(jnp.float32))
    spread_rows(hi_b, (bins // both).astype(jnp.float32))
    spread_rows(part_b, ((bins % both) // width).astype(jnp.float32))
    tops = local_tops(lw, bins)
    low, high = bins % LANES, bins // LANES
    own_top = jnp.zeros(lw.shape, jnp.float32)
    for t in range(BINS // LANES):
        picked = jnp.take_along_axis(jnp.broadcast_to(tops[t:t + 1], lw.shape), low, axis=1)
        own_top = jnp.where(high == t, picked, own_top)
        top_tab[t] = jnp.broadcast_to(tops[t:t + 1], (8, LANES))
    spread_rows(w_b, jnp.exp(lw - own_top))
    load.wait()

    zero = jnp.zeros((), jnp.bfloat16)
    one_label = lax.broadcasted_iota(jnp.int32, (EXTRA, LANES), 0) // (EXTRA // split)
    one_label = one_label.astype(jnp.float32).astype(jnp.bfloat16)

    def mask_states(r, carry):
        part = part_b[pl.ds(pl.multiple_of(r * 16, 16), 16), :]
        cols = pl.ds(pl.multiple_of(r * LANES, LANES), LANES)
        tile = held[:, cols]
        part_all = jnp.concatenate([part] * (state // 16), axis=0)
        for q in range(split):
            ext[q * state:(q + 1) * state, cols] = jnp.where(part_all == jnp.bfloat16(q), tile, zero)
        ext[split * state:split * state + EXTRA, cols] = jnp.where(part == one_label, jnp.bfloat16(1), zero)
        return carry

    lax.fori_loop(0, rows, mask_states, 0)
    pl.semaphore_wait(barrier, groups - 1)

    depth = 16
    label = lax.broadcasted_iota(jnp.int32, (width, LANES), 0).astype(jnp.float32).astype(jnp.bfloat16)

    def block(dest, out):
        tile = dest.astype(jnp.float32).astype(jnp.bfloat16)

        def step(c, carry):
            pieces = []
            for j in range(depth):
                at = pl.ds(pl.multiple_of((c * depth + j) * 16, 16), 16)
                w = jnp.where(hi_b[at, :] == tile, w_b[at, :], zero)
                lo = lo_b[at, :]
                w_all = jnp.concatenate([w] * (width // 16), axis=0)
                lo_all = jnp.concatenate([lo] * (width // 16), axis=0)
                pieces.append(jnp.where(lo_all == label, w_all, zero))
            spread = jnp.concatenate(pieces, axis=1)
            cols = pl.ds(pl.multiple_of(c * depth * LANES, LANES), depth * LANES)
            out[...] += lax.dot_general(ext[:, cols], spread, (((1,), (1,)), ((), ())),
                                        preferred_element_type=jnp.float32)
            return carry

        out[...] = jnp.zeros(out.shape, jnp.float32)
        lax.fori_loop(0, rows // depth, step, 0)

    half = split // 2

    def part_of(found, which, p):
        sums = found[pl.ds(pl.multiple_of((which * half + p) * state, state), state), :]
        at = split * state + p * (EXTRA // split)
        first = found[at:at + 1, :]
        at = at + half * (EXTRA // split)
        return sums, jnp.where(which == 0, first, found[at:at + 1, :])

    def tops_of(owner, p):
        tiles = [top_tab[(owner * half + p) * (width // LANES) + t] for t in range(width // LANES)]
        return jnp.concatenate(tiles, axis=1)

    order = sorted(range(1, chips), key=lambda m: -min(m, chips - m)) + [0]
    pair_copies, chip_copies = [], []
    for s, m in enumerate(order):
        dest = lax.rem(chip + m, chips)
        found = blocks.at[s]
        block(dest, found)
        for p in range(half):
            lanes = slice(p * width, (p + 1) * width)
            sums, mass = part_of(found, 1 - core, p)
            pair_send[s, 0:state, lanes] = sums
            pair_send[s, state:state + 4, lanes] = jnp.broadcast_to(mass, (4, width))
            pair_send[s, state + 4:state + 8, lanes] = tops_of(dest * 2 + 1 - core, p)[0:4]
        copy = pltpu.make_async_remote_copy(
            pair_send.at[s], pair_recv.at[s], pair_ss.at[s], pair_rs.at[s],
            device_id={"dom": partner}, device_id_type=pl.DeviceIdType.MESH)
        copy.start()
        pair_copies.append(copy)
        copy.wait_recv()
        for p in range(half):
            lanes = slice(p * width, (p + 1) * width)
            sums, mass = part_of(found, core, p)
            mine = tops_of(dest * 2 + core, p)[0:4]
            theirs = pair_recv[s, state + 4:state + 8, lanes]
            top = jnp.maximum(mine, theirs)
            by_mine, by_theirs = jnp.exp(mine - top), jnp.exp(theirs - top)
            chip_send[s, 0:state, lanes] = sums * by_mine[0:1] + pair_recv[s, 0:state, lanes] * by_theirs[0:1]
            chip_send[s, state:state + 4, lanes] = mass * by_mine + pair_recv[s, state:state + 4, lanes] * by_theirs
            chip_send[s, state + 4:state + 8, lanes] = top
        if m:
            copy = pltpu.make_async_remote_copy(
                chip_send.at[s], chip_recv.at[s], chip_ss.at[s], chip_rs.at[s],
                device_id={"dom": dest * 2 + core}, device_id_type=pl.DeviceIdType.MESH)
            copy.start()
            chip_copies.append(copy)

    for copy in chip_copies:
        copy.wait_recv()
    last = chips - 1
    tops = [chip_send[last, state + 4:state + 5, :]] + [chip_recv[s, state + 4:state + 5, :] for s in range(last)]
    bin_top = functools.reduce(jnp.maximum, tops)
    sums = chip_send[last, 0:state + 8, :] * jnp.exp(tops[0] - bin_top)
    for s in range(last):
        sums = sums + chip_recv[s, 0:state + 8, :] * jnp.exp(tops[s + 1] - bin_top)
    mass = sums[state:state + 1, :]
    block_top = jnp.max(bin_top, axis=1, keepdims=True)
    block_mass = jnp.sum(mass * jnp.exp(bin_top - block_top), axis=1, keepdims=True)
    stat_send[0:4, :] = jnp.broadcast_to(block_top, (4, LANES))
    stat_send[4:8, :] = jnp.broadcast_to(block_mass, (4, LANES))
    stat_copies = []
    for k in range(1, groups):
        copy = pltpu.make_async_remote_copy(
            stat_send, stat_recv.at[k - 1], stat_ss.at[k - 1], stat_rs.at[k - 1],
            device_id={"dom": lax.rem(me + k, groups)}, device_id_type=pl.DeviceIdType.MESH)
        copy.start()
        stat_copies.append(copy)
    means_ref[...] = sums[0:state] / jnp.maximum(mass, 1.0)
    for copy in stat_copies:
        copy.wait_recv()
    top = block_top
    for k in range(groups - 1):
        top = jnp.maximum(top, stat_recv[k, 0:1, 0:1])
    total = block_mass * jnp.exp(block_top - top)
    before = jnp.zeros_like(total)
    for k in range(groups - 1):
        theirs = stat_recv[k, 4:5, 0:1] * jnp.exp(stat_recv[k, 0:1, 0:1] - top)
        total = total + theirs
        before = before + jnp.where(me >= k + 1, theirs, 0.0)
    share = mass * jnp.exp(bin_top - top)
    position = lax.broadcasted_iota(jnp.int32, share.shape, 1)
    run = share
    hop = 1
    while hop < owned:
        run = run + jnp.where(position >= hop, pltpu.roll(run, hop, 1), 0.0)
        hop *= 2
    cum_ref[...] = (before + run) / total
    weights_ref[...] = whole_count * jnp.exp(lw - top) / total
    for copy in pair_copies + chip_copies + stat_copies:
        copy.wait_send()


def body(log_weights, bins, states):
    groups = lax.axis_size("dom")
    owned = BINS // groups
    chips = groups // 2
    state, count = states.shape
    rows = count // LANES
    width = min(256, owned)
    split = 2 * owned // width
    vmem = pl.BlockSpec(memory_space=pltpu.VMEM)
    blocks = pltpu.VMEM((chips, state + 8, owned), jnp.float32)
    cumulative, bin_means, weights = pl.pallas_call(
        functools.partial(kernel, groups, float(count * groups)),
        out_shape=(jax.ShapeDtypeStruct((1, owned), jnp.float32),
                   jax.ShapeDtypeStruct((state, owned), jnp.float32),
                   jax.ShapeDtypeStruct((rows, LANES), jnp.float32)),
        in_specs=[vmem, vmem, pl.BlockSpec(memory_space=pl.ANY)],
        out_specs=(vmem, vmem, vmem),
        scratch_shapes=[
            pltpu.VMEM((state, count), jnp.bfloat16),
            pltpu.VMEM((split * state + EXTRA, count), jnp.bfloat16),
            pltpu.VMEM((rows * 16, LANES), jnp.bfloat16),
            pltpu.VMEM((rows * 16, LANES), jnp.bfloat16),
            pltpu.VMEM((rows * 16, LANES), jnp.bfloat16),
            pltpu.VMEM((rows * 16, LANES), jnp.bfloat16),
            pltpu.VMEM((BINS // LANES, 8, LANES), jnp.float32),
            pltpu.VMEM((chips, split * state + EXTRA, width), jnp.float32),
            blocks, blocks, blocks, blocks,
            pltpu.VMEM((8, LANES), jnp.float32),
            pltpu.VMEM((groups - 1, 8, LANES), jnp.float32),
            pltpu.SemaphoreType.DMA,
            pltpu.SemaphoreType.DMA((chips,)),
            pltpu.SemaphoreType.DMA((chips,)),
            pltpu.SemaphoreType.DMA((chips,)),
            pltpu.SemaphoreType.DMA((chips,)),
            pltpu.SemaphoreType.DMA((groups - 1,)),
            pltpu.SemaphoreType.DMA((groups - 1,)),
        ],
        compiler_params=pltpu.CompilerParams(
            collective_id=0, has_side_effects=True, vmem_limit_bytes=48 * 1024 * 1024),
    )(log_weights.reshape(rows, LANES), bins.reshape(rows, LANES), states)
    return cumulative.reshape(owned), bin_means, weights.reshape(count)


def solution(mesh):
    placed = (P(("filt", "dom")), P(("filt", "dom")), P(None, ("filt", "dom")))
    return jax.shard_map(
        body,
        mesh=mesh,
        in_specs=placed,
        out_specs=(P(("filt", "dom")), P(None, ("filt", "dom")), P(("filt", "dom"))),
        check_vma=False,
    )
```
